32 devices in a mesh: clip: 2 (over y), rows: 8 (over z, x), tm: 2 (over core).
Axes of the slice: x: 2, y: 2, z: 4, core: 2. Of those that a mesh axis runs over, the one named last changes fastest.
Arguments:
- latent: bfloat16 [8, 8, 64, 192], P(('clip', 'tm'), 'rows'), parts along dimension 0, may hold values from -18 to 18
- gain_first: bfloat16 [192], replicated, may hold values from 0.099609375 to 1.8984375
- conv_first: bfloat16 [3, 3, 3, 192, 192], replicated, may hold values from -0.078125 to 0.078125
- gain_second: bfloat16 [192], replicated, may hold values from 0.099609375 to 1.8984375
- conv_second: bfloat16 [3, 3, 3, 192, 192], replicated, may hold values from -0.078125 to 0.078125
- conv_up: bfloat16 [3, 3, 96, 192], replicated, may hold values from -0.15625 to 0.15625
Outputs:
- decoded: bfloat16 [8, 16, 96, 128], P(('clip', 'tm'), 'rows'), parts along dimension 0
- peaks: float32 [6, 192], P('clip'), parts along dimension 0
The draws below stay inside these ranges and needn't reach their ends.
There are 2 independent parts, one for each index of `clip`. The reference program is written for one: setup_inputs(seed, part) draws one part's arguments, and reference() takes and returns one part's arrays. A program takes and returns all parts, laid end to end along the dimension named above; an argument that names none is the same for every part. Nothing has to cross between parts.
All inputs are finite; a program needn't handle non-finite values.
Results may differ from the reference program's by a relative error of at most 0.0085.
Values may be sent and summed in bfloat16 or wider, within the bound.
A program may use at most 64 MiB of HBM per device.

```python
import math
import jax
import jax.numpy as jnp
from jax import lax

C = 192
C2 = 96
COLS = 64
FRAMES = 4
ROWS = 8


def draw_latent(key, part):
    base_key = jax.random.fold_in(key, 11)
    noise_key, spread_key = jax.random.split(base_key)
    spread = jnp.exp(jax.random.uniform(spread_key, (1, ROWS, 1, C), jnp.float32, math.log(0.3), math.log(3.0)))
    rising = 0.5 + jnp.arange(ROWS, dtype=jnp.float32).reshape(1, ROWS, 1, 1) / ROWS
    noise = jnp.clip(jax.random.normal(noise_key, (FRAMES, ROWS, COLS, C), jnp.float32), -4.0, 4.0)
    return (noise * spread * rising).astype(jnp.bfloat16)


def scatter_about(own_key, dims, deviation, most, kind=jnp.bfloat16):
    entries = jax.random.normal(own_key, dims, jnp.float32) * deviation
    return jnp.minimum(jnp.maximum(entries, -most), most).astype(kind)


def setup_inputs(seed: int = 0, part: int = 0) -> dict:
    splits = jax.random.split(jax.random.key(seed), 7)
    part_splits = jax.random.split(jax.random.fold_in(splits[6], part), 7)
    latent = draw_latent(jax.random.fold_in(jax.random.fold_in(splits[6], part), 71), part)
    gain_first = jnp.clip(1.0 + 0.18 * jax.random.normal(splits[1], (C,), jnp.float32), 0.099609375, 1.8984375).astype(jnp.bfloat16)
    conv_first = scatter_about(splits[2], (3, 3, 3, C, C), (27 * C) ** -0.5, 0.078125)
    gain_second = jnp.clip(1.0 + 0.18 * jax.random.normal(splits[3], (C,), jnp.float32), 0.099609375, 1.8984375).astype(jnp.bfloat16)
    conv_second = scatter_about(splits[4], (3, 3, 3, C, C), (27 * C) ** -0.5, 0.078125)
    conv_up = scatter_about(splits[5], (3, 3, C2, C), (9 * C) ** -0.5, 0.15625)
    return {"latent": latent, "gain_first": gain_first, "conv_first": conv_first, "gain_second": gain_second, "conv_second": conv_second, "conv_up": conv_up}


def rms_norm(values, gain):
    floats = values.astype(jnp.float32)
    scale = lax.rsqrt(lax.optimization_barrier(jnp.mean(floats * floats, axis=-1, keepdims=True)) + 1e-06)
    return floats * scale * gain.astype(jnp.float32)

def causal_taps(extended, weights, frame_count, row_count, col_count):
    channels = extended.shape[-1]
    total = jnp.zeros((frame_count * row_count * col_count, weights.shape[-1]), jnp.float32)
    for time_tap in range(3):
        for row_tap in range(3):
            sliced = extended[time_tap:time_tap + frame_count, row_tap:row_tap + row_count]
            stacked = jnp.concatenate([sliced[:, :, col_tap:col_tap + col_count] for col_tap in range(3)], axis=-1)
            matrix = weights[time_tap, row_tap].reshape(3 * channels, weights.shape[-1])
            total = total + jnp.dot(stacked.reshape(-1, 3 * channels), matrix, preferred_element_type=jnp.float32)
    return total.reshape(frame_count, row_count, col_count, weights.shape[-1])

def plane_taps(wide_padded, conv_up, row_count, col_count):
    channels = wide_padded.shape[-1]
    frame_count = wide_padded.shape[0]
    total = jnp.zeros((frame_count * row_count * col_count, conv_up.shape[2]), jnp.float32)
    for row_tap in range(3):
        sliced = wide_padded[:, row_tap:row_tap + row_count]
        stacked = jnp.concatenate([sliced[:, :, col_tap:col_tap + col_count] for col_tap in range(3)], axis=-1)
        matrix = jnp.transpose(conv_up[row_tap], (0, 2, 1)).reshape(3 * channels, conv_up.shape[2])
        total = total + jnp.dot(stacked.reshape(-1, 3 * channels), matrix, preferred_element_type=jnp.float32)
    output = total.reshape(frame_count, row_count, col_count, conv_up.shape[2])
    return jnp.transpose(output, (0, 1, 3, 2)).astype(jnp.bfloat16)

def channel_peak(values):
    return lax.optimization_barrier(jnp.max(jnp.abs(values).astype(jnp.float32), axis=(0, 1, 2)))

def causal_whole(values, weights):
    frame_count, row_count, col_count = (values.shape[0], values.shape[1], values.shape[2])
    extended = jnp.pad(values, ((2, 0), (1, 1), (1, 1), (0, 0)))
    return causal_taps(extended, weights, frame_count, row_count, col_count)

def reference(latent, gain_first, conv_first, gain_second, conv_second, conv_up):
    first = jax.nn.silu(rms_norm(latent, gain_first)).astype(jnp.bfloat16)
    hidden = causal_whole(first, conv_first).astype(jnp.bfloat16)
    second = jax.nn.silu(rms_norm(hidden, gain_second)).astype(jnp.bfloat16)
    merged = (latent.astype(jnp.float32) + causal_whole(second, conv_second)).astype(jnp.bfloat16)
    row_count, col_count = (merged.shape[1], merged.shape[2])

    def one_frame(frame):
        wide = jnp.repeat(jnp.repeat(frame[None], 2, axis=1), 2, axis=2)
        wide = jnp.pad(wide, ((0, 0), (1, 1), (1, 1), (0, 0)))
        return plane_taps(wide, conv_up, 2 * row_count, 2 * col_count)[0]
    decoded = lax.map(one_frame, merged)
    peaks = jnp.stack([channel_peak(first), channel_peak(second), channel_peak(merged)], axis=0)
    return (decoded, peaks)
```

```python
import functools

import jax
import jax.numpy as jnp
from jax import lax
from jax.experimental import pallas as pl
from jax.experimental.pallas import tpu as pltpu
from jax.sharding import PartitionSpec as P

MESH = pl.DeviceIdType.MESH
BF16 = jnp.bfloat16
F32 = jnp.float32
REACH = 2


def normed_silu(values, gain):
    scale = lax.rsqrt(jnp.mean(values * values, axis=-1, keepdims=True) + 1e-06)
    u = values * scale * gain
    return (u / (1.0 + jnp.exp(-u))).astype(BF16)


def peak_of(values):
    return jnp.max(jnp.abs(values.astype(F32)), axis=0, keepdims=True)


def dot(a, b):
    return jnp.dot(a, b, preferred_element_type=F32)


def dot_nt(a, b):
    return lax.dot_general(a, b, (((1,), (1,)), ((), ())), preferred_element_type=F32)


def taps_sum(buf, weights, frames, rows_out, cols):
    depth = buf.shape[-1]
    pixels = frames * rows_out * cols
    lhs = jnp.concatenate(
        [
            buf[i : i + frames, j * cols : (j + rows_out) * cols, :].reshape(pixels, depth)
            for i in range(3)
            for j in range(3)
        ],
        axis=1,
    )
    parts = []
    for k in range(3):
        rhs = jnp.concatenate([weights[ij * 3 + k] for ij in range(9)], axis=0)
        parts.append(dot(lhs, rhs))
    col = lax.rem(lax.broadcasted_iota(jnp.int32, parts[0].shape, 0), cols)
    left = jnp.where(col == 0, 0.0, pltpu.roll(parts[0], 1, 0))
    right = jnp.where(col == cols - 1, 0.0, pltpu.roll(parts[2], pixels - 1, 0))
    return left + parts[1] + right


def kernel(
    R, T, lat_hbm, g1_ref, w1_hbm, g2_ref, w2_hbm, up_hbm, dec_ref, peaks_ref,
    lat, prev, first, second, w1, w2, up, merged, pk_send, pk_recv,
    load_sem, x1_send, x1_recv, rl_send, rl_recv, s_send, s_recv, x3_send, x3_recv, pk_ssem, pk_rsem,
):
    r = lax.axis_index("rows")
    t = lax.axis_index("tm")
    n = R * T
    me = r * T + t
    _, frames, cols, C = lat.shape
    half = pk_send.shape[-1]
    SPAN = 2 * REACH + 1

    loads = [
        pltpu.make_async_copy(lat_hbm, lat.at[REACH], load_sem.at[0]),
        pltpu.make_async_copy(w1_hbm, w1.at[:, 0:C, :], load_sem.at[1]),
        pltpu.make_async_copy(w2_hbm, w2.at[:, 0:C, :], load_sem.at[2]),
        pltpu.make_async_copy(up_hbm, up, load_sem.at[3]),
    ]
    for copy in loads:
        copy.start()

    barrier = pltpu.get_barrier_semaphore()

    def greet(k, carry):
        peer = lax.rem(me + k, n)
        pl.semaphore_signal(
            barrier, inc=1, device_id={"rows": peer // T, "tm": lax.rem(peer, T)}, device_id_type=MESH
        )
        return carry

    second[frames:, :, :] = jnp.zeros_like(second[frames:, :, :])

    @pl.when(t == 0)
    def _():
        second[0:frames, :, :] = jnp.zeros_like(second[0:frames, :, :])

    @pl.when(r == 0)
    def _():
        merged[0] = jnp.zeros_like(merged[0])

    @pl.when(r == R - 1)
    def _():
        merged[2] = jnp.zeros_like(merged[2])

    lax.fori_loop(1, n, greet, 0, unroll=n <= 16)

    first[...] = jnp.zeros_like(first)
    pad = w1.shape[1] - C
    w1[:, C:, :] = jnp.zeros((w1.shape[0], pad, C), BF16)
    w2[:, C:, :] = jnp.zeros((w2.shape[0], pad, C), BF16)
    pk_send[...] = jnp.zeros_like(pk_send)

    loads[0].wait()
    pl.semaphore_wait(barrier, n - 1)

    offsets = [1, -1, 2, -2]

    def row_copy(d):
        slot = REACH - d
        return pltpu.make_async_remote_copy(
            src_ref=lat.at[REACH], dst_ref=lat.at[slot], send_sem=x1_send.at[slot],
            recv_sem=x1_recv.at[slot], device_id={"rows": r + d}, device_id_type=MESH,
        )

    def there(d):
        return jnp.logical_and(r + d >= 0, r + d < R)

    for d in offsets:
        pl.when(there(d))(lambda d=d: row_copy(d).start())

    def relay(slot):
        return pltpu.make_async_remote_copy(
            src_ref=lat.at[slot], dst_ref=prev.at[slot], send_sem=rl_send.at[slot],
            recv_sem=rl_recv.at[slot], device_id={"tm": t + 1}, device_id_type=MESH,
        )

    gives = t < T - 1
    takes = t > 0
    pl.when(gives)(lambda: relay(REACH).start())

    gain1 = g1_ref[...].astype(F32)
    gain2 = g2_ref[...].astype(F32)

    def put_first(source, slot, at):
        rows = slice(slot * cols, (slot + 1) * cols)
        values = normed_silu(source[slot].astype(F32).reshape(frames * cols, C), gain1)
        first[at : at + frames, rows, 0:C] = values.reshape(frames, cols, C)
        return values

    def put_peak(i, row):
        pk_send[2 * i : 2 * i + 1, :] = row[:, 0:half]
        pk_send[2 * i + 1 : 2 * i + 2, 0 : C - half] = row[:, half:C]

    put_peak(0, peak_of(put_first(lat, REACH, frames)))

    for d in offsets:
        slot = REACH + d

        @pl.when(there(d))
        def _(d=d, slot=slot):
            row_copy(-d).wait_recv()
            pl.when(gives)(lambda: relay(slot).start())
            put_first(lat, slot, frames)

    @pl.when(takes)
    def _():
        for d in [0] + offsets:
            slot = REACH + d

            @pl.when(there(d))
            def _(slot=slot):
                relay(slot).wait_recv()
                put_first(prev, slot, 0)

    loads[1].wait()
    hidden = taps_sum(first, w1, frames, 3, cols).astype(BF16).astype(F32)
    activated = normed_silu(hidden, gain2).reshape(frames, 3, cols, C)
    zeros = jnp.zeros((frames, cols, C), BF16)
    for j in range(3):
        values = activated[:, j]
        if j != 1:
            values = jnp.where(there(j - 1), values, zeros)
        second[frames:, j * cols : (j + 1) * cols, 0:C] = values

    def hand_on():
        return pltpu.make_async_remote_copy(
            src_ref=second.at[pl.ds(frames, frames)], dst_ref=second.at[pl.ds(0, frames)],
            send_sem=s_send, recv_sem=s_recv, device_id={"tm": t + 1}, device_id_type=MESH,
        )

    pl.when(gives)(lambda: hand_on().start())
    put_peak(1, peak_of(activated[:, 1].reshape(frames * cols, C)))
    loads[2].wait()
    pl.when(takes)(lambda: hand_on().wait_recv())

    block = lat[REACH].astype(F32).reshape(frames * cols, C) + taps_sum(second, w2, frames, 1, cols)
    block = block.astype(BF16)
    merged[1] = block.reshape(frames, cols, C)
    put_peak(2, peak_of(block))

    def edge_copy(d):
        slot = 1 - d
        return pltpu.make_async_remote_copy(
            src_ref=merged.at[1], dst_ref=merged.at[slot], send_sem=x3_send.at[slot],
            recv_sem=x3_recv.at[slot], device_id={"rows": r + d}, device_id_type=MESH,
        )

    for d in (1, -1):
        pl.when(there(d))(lambda d=d: edge_copy(d).start())

    def peak_copy(k):
        peer = lax.rem(me + k, n)
        return pltpu.make_async_remote_copy(
            src_ref=pk_send, dst_ref=pk_recv.at[k], send_sem=pk_ssem.at[k], recv_sem=pk_rsem.at[k],
            device_id={"rows": peer // T, "tm": lax.rem(peer, T)}, device_id_type=MESH,
        )

    def send_peak(k, carry):
        peak_copy(k).start()
        return carry

    lax.fori_loop(1, n, send_peak, 0, unroll=n <= 16)

    loads[3].wait()
    C2 = dec_ref.shape[2]
    width = frames * cols
    own = dot_nt(up[...], block).reshape(3, 3, C2, width)
    upper = own[1] + own[2]
    lower = own[0] + own[1]
    for d in (1, -1):
        pl.when(there(d))(lambda d=d: edge_copy(-d).wait_recv())
    upper = upper + dot_nt(up[0 : 3 * C2], merged[0].reshape(width, C)).reshape(3, C2, width)
    lower = lower + dot_nt(up[6 * C2 :], merged[2].reshape(width, C)).reshape(3, C2, width)
    lane = lax.rem(lax.broadcasted_iota(jnp.int32, (C2, width), 1), cols)

    def columns(sums):
        from_left = jnp.where(lane == 0, 0.0, pltpu.roll(sums[0], 1, 1))
        from_right = jnp.where(lane == cols - 1, 0.0, pltpu.roll(sums[2], width - 1, 1))
        even = from_left + sums[1] + sums[2]
        odd = sums[0] + sums[1] + from_right
        return jnp.concatenate([even, odd], axis=1).astype(BF16)

    narrow = jnp.concatenate([columns(upper), columns(lower)], axis=0)
    q = lax.broadcasted_iota(jnp.int32, (2 * width, 2 * width), 0)
    o = lax.broadcasted_iota(jnp.int32, (2 * width, 2 * width), 1)
    frame = lax.rem(lax.div(q, cols), frames)
    target = frame * (2 * cols) + 2 * lax.rem(q, cols) + lax.div(q, width)
    spread = jnp.where(o == target, 1.0, 0.0).astype(BF16)
    wide = dot(narrow, spread).astype(BF16)
    for f in range(frames):
        for j in range(2):
            dec_ref[f, j] = wide[j * C2 : (j + 1) * C2, f * 2 * cols : (f + 1) * 2 * cols]

    def take_peak(k, best):
        peak_copy(k).wait_recv()
        return jnp.maximum(best, pk_recv[k])

    best = lax.fori_loop(1, n, take_peak, pk_send[...], unroll=n <= 16)
    for i in range(3):
        peaks_ref[i : i + 1, 0:half] = best[2 * i : 2 * i + 1, :]
        peaks_ref[i : i + 1, half:C] = best[2 * i + 1 : 2 * i + 2, 0 : C - half]

    def end_peak(k, carry):
        peak_copy(k).wait_send()
        return carry

    lax.fori_loop(1, n, end_peak, 0, unroll=n <= 16)
    for d in offsets:
        pl.when(there(d))(lambda d=d: row_copy(d).wait_send())
    for d in (1, -1):
        pl.when(there(d))(lambda d=d: edge_copy(d).wait_send())

    @pl.when(gives)
    def _():
        for d in [0] + offsets:
            pl.when(there(d))(lambda d=d: relay(REACH + d).wait_send())
        hand_on().wait_send()


def per_device(latent, gain_first, conv_first, gain_second, conv_second, conv_up):
    frames, rows, cols, C = latent.shape
    R, T = lax.axis_size("rows"), lax.axis_size("tm")
    C2 = conv_up.shape[2]
    n = R * T
    if rows != 1 or frames != 2:
        raise ValueError("unsupported block")
    half = 128
    depth = -(-C // 256) * 256
    taps = 27
    vmem = pl.BlockSpec(memory_space=pltpu.VMEM)
    hbm = pl.BlockSpec(memory_space=pl.ANY)
    dma = pltpu.SemaphoreType.DMA
    return pl.pallas_call(
        functools.partial(kernel, R, T),
        out_shape=(
            jax.ShapeDtypeStruct((frames, 2 * rows, C2, 2 * cols), BF16),
            jax.ShapeDtypeStruct((3, C), F32),
        ),
        in_specs=[hbm, vmem, hbm, vmem, hbm, hbm],
        out_specs=(vmem, vmem),
        scratch_shapes=[
            pltpu.VMEM((2 * REACH + 1, frames, cols, C), BF16),
            pltpu.VMEM((2 * REACH + 1, frames, cols, C), BF16),
            pltpu.VMEM((2 * frames, (2 * REACH + 1) * cols, depth), BF16),
            pltpu.VMEM((2 * frames, 3 * cols, depth), BF16),
            pltpu.VMEM((taps, depth, C), BF16),
            pltpu.VMEM((taps, depth, C), BF16),
            pltpu.VMEM((9 * C2, C), BF16),
            pltpu.VMEM((3, frames, cols, C), BF16),
            pltpu.VMEM((8, half), F32),
            pltpu.VMEM((n, 8, half), F32),
            dma((4,)),
            dma((2 * REACH + 1,)),
            dma((2 * REACH + 1,)),
            dma((2 * REACH + 1,)),
            dma((2 * REACH + 1,)),
            dma,
            dma,
            dma((3,)),
            dma((3,)),
            dma((n,)),
            dma((n,)),
        ],
        compiler_params=pltpu.CompilerParams(collective_id=0, has_side_effects=True),
    )(
        latent.reshape(frames, cols, C),
        gain_first.reshape(1, C),
        conv_first.reshape(taps, C, C),
        gain_second.reshape(1, C),
        conv_second.reshape(taps, C, C),
        conv_up.reshape(9 * C2, C),
    )


def solution(mesh):
    return jax.shard_map(
        per_device,
        mesh=mesh,
        in_specs=(P(("clip", "tm"), "rows", None, None), P(), P(), P(), P(), P()),
        out_specs=(P(("clip", "tm"), "rows", None, None), P("clip", None)),
        check_vma=False,
    )
```

```python
import functools

import jax
import jax.numpy as jnp
from jax import lax
from jax.experimental import pallas as pl
from jax.experimental.pallas import tpu as pltpu
from jax.sharding import PartitionSpec as P

MESH = pl.DeviceIdType.MESH
BF16 = jnp.bfloat16
F32 = jnp.float32
REACH = 2


def normed_silu(values, gain):
    scale = lax.rsqrt(jnp.mean(values * values, axis=-1, keepdims=True) + 1e-06)
    u = values * scale * gain
    return (u / (1.0 + jnp.exp(-u))).astype(BF16)


def peak_of(values):
    return jnp.max(jnp.abs(values.astype(F32)), axis=0, keepdims=True)


def dot(a, b):
    return jnp.dot(a, b, preferred_element_type=F32)


def dot_nt(a, b):
    return lax.dot_general(a, b, (((1,), (1,)), ((), ())), preferred_element_type=F32)


def taps_sum(buf, weights, frames, rows_out, cols):
    depth = buf.shape[-1]
    pixels = frames * rows_out * cols
    lhs = jnp.concatenate(
        [
            buf[i : i + frames, j * cols : (j + rows_out) * cols, :].reshape(pixels, depth)
            for i in range(3)
            for j in range(3)
        ],
        axis=1,
    )
    parts = []
    for k in range(3):
        rhs = jnp.concatenate([weights[ij * 3 + k] for ij in range(9)], axis=0)
        parts.append(dot(lhs, rhs))
    col = lax.rem(lax.broadcasted_iota(jnp.int32, parts[0].shape, 0), cols)
    left = jnp.where(col == 0, 0.0, pltpu.roll(parts[0], 1, 0))
    right = jnp.where(col == cols - 1, 0.0, pltpu.roll(parts[2], pixels - 1, 0))
    return left + parts[1] + right


def kernel(
    R, T, lat_hbm, g1_ref, w1_hbm, g2_ref, w2_hbm, up_hbm, dec_ref, peaks_ref,
    lat, prev, first, second, w1, w2, up, merged, pk_send, pk_recv,
    load_sem, x1_send, x1_recv, rl_send, rl_recv, s_send, s_recv, x3_send, x3_recv, pk_ssem, pk_rsem, known,
):
    r = lax.axis_index("rows")
    t = lax.axis_index("tm")
    n = R * T
    me = r * T + t
    _, frames, cols, C = lat.shape
    half = pk_send.shape[-1]
    SPAN = 2 * REACH + 1

    loads = [
        pltpu.make_async_copy(lat_hbm, lat.at[REACH], load_sem.at[0]),
        pltpu.make_async_copy(w1_hbm, w1.at[:, 0:C, :], load_sem.at[1]),
        pltpu.make_async_copy(w2_hbm, w2.at[:, 0:C, :], load_sem.at[2]),
        pltpu.make_async_copy(up_hbm, up, load_sem.at[3]),
    ]
    for copy in loads:
        copy.start()

    barrier = pltpu.get_barrier_semaphore()

    def there(d):
        return jnp.logical_and(r + d >= 0, r + d < R)

    near = [(d, e) for d in range(-REACH, REACH + 1) for e in range(T) if (d, e) != (0, 0)]

    def greet(d, e):
        pl.semaphore_signal(
            barrier, inc=1, device_id={"rows": r + d, "tm": lax.rem(t + e, T)}, device_id_type=MESH
        )

    second[frames:, :, :] = jnp.zeros_like(second[frames:, :, :])

    @pl.when(t == 0)
    def _():
        second[0:frames, :, :] = jnp.zeros_like(second[0:frames, :, :])

    @pl.when(r == 0)
    def _():
        merged[0] = jnp.zeros_like(merged[0])

    @pl.when(r == R - 1)
    def _():
        merged[2] = jnp.zeros_like(merged[2])

    for d, e in near:
        pl.when(there(d))(functools.partial(greet, d, e))

    first[...] = jnp.zeros_like(first)
    pad = w1.shape[1] - C
    w1[:, C:, :] = jnp.zeros((w1.shape[0], pad, C), BF16)
    w2[:, C:, :] = jnp.zeros((w2.shape[0], pad, C), BF16)
    pk_send[...] = jnp.zeros_like(pk_send)

    loads[0].wait()
    rows_near = 1 + jnp.minimum(r, REACH) + jnp.minimum(R - 1 - r, REACH)
    pl.semaphore_wait(barrier, rows_near * T - 1)

    offsets = [1, -1, 2, -2]

    def row_copy(d):
        slot = REACH - d
        return pltpu.make_async_remote_copy(
            src_ref=lat.at[REACH], dst_ref=lat.at[slot], send_sem=x1_send.at[slot],
            recv_sem=x1_recv.at[slot], device_id={"rows": r + d}, device_id_type=MESH,
        )

    for d in offsets:
        pl.when(there(d))(lambda d=d: row_copy(d).start())

    stages = [REACH << i for i in range(R.bit_length()) if (REACH << i) < R - 1]

    def tell(i):
        for side, d in enumerate((stages[i], -stages[i])):
            pl.when(there(d))(
                lambda side=side, d=d: pl.semaphore_signal(
                    known.at[i, side], inc=1, device_id={"rows": r + d}, device_id_type=MESH
                )
            )

    def hear(i):
        for side, d in enumerate((stages[i], -stages[i])):
            pl.when(there(-d))(lambda side=side: pl.semaphore_wait(known.at[i, side], 1))

    if stages:
        tell(0)

    def relay(slot):
        return pltpu.make_async_remote_copy(
            src_ref=lat.at[slot], dst_ref=prev.at[slot], send_sem=rl_send.at[slot],
            recv_sem=rl_recv.at[slot], device_id={"tm": t + 1}, device_id_type=MESH,
        )

    gives = t < T - 1
    takes = t > 0
    pl.when(gives)(lambda: relay(REACH).start())

    gain1 = g1_ref[...].astype(F32).reshape(1, C)
    gain2 = g2_ref[...].astype(F32).reshape(1, C)

    def put_first(source, slot, at):
        rows = slice(slot * cols, (slot + 1) * cols)
        values = normed_silu(source[slot].astype(F32).reshape(frames * cols, C), gain1)
        first[at : at + frames, rows, 0:C] = values.reshape(frames, cols, C)
        return values

    def put_peak(i, row):
        pk_send[2 * i : 2 * i + 1, :] = row[:, 0:half]
        pk_send[2 * i + 1 : 2 * i + 2, 0 : C - half] = row[:, half:C]

    put_peak(0, peak_of(put_first(lat, REACH, frames)))

    for d in offsets:
        slot = REACH + d

        @pl.when(there(d))
        def _(d=d, slot=slot):
            row_copy(-d).wait_recv()
            pl.when(gives)(lambda: relay(slot).start())
            put_first(lat, slot, frames)

    for i in range(1, len(stages)):
        hear(i - 1)
        tell(i)

    @pl.when(takes)
    def _():
        for d in [0] + offsets:
            slot = REACH + d

            @pl.when(there(d))
            def _(slot=slot):
                relay(slot).wait_recv()
                put_first(prev, slot, 0)

    loads[1].wait()
    hidden = taps_sum(first, w1, frames, 3, cols).astype(BF16).astype(F32)
    activated = normed_silu(hidden, gain2).reshape(frames, 3, cols, C)
    zeros = jnp.zeros((frames, cols, C), BF16)
    for j in range(3):
        values = activated[:, j]
        if j != 1:
            values = jnp.where(there(j - 1), values, zeros)
        second[frames:, j * cols : (j + 1) * cols, 0:C] = values

    def hand_on():
        return pltpu.make_async_remote_copy(
            src_ref=second.at[pl.ds(frames, frames)], dst_ref=second.at[pl.ds(0, frames)],
            send_sem=s_send, recv_sem=s_recv, device_id={"tm": t + 1}, device_id_type=MESH,
        )

    pl.when(gives)(lambda: hand_on().start())
    put_peak(1, peak_of(activated[:, 1].reshape(frames * cols, C)))
    loads[2].wait()
    pl.when(takes)(lambda: hand_on().wait_recv())

    block = lat[REACH].astype(F32).reshape(frames * cols, C) + taps_sum(second, w2, frames, 1, cols)
    block = block.astype(BF16)
    merged[1] = block.reshape(frames, cols, C)
    put_peak(2, peak_of(block))

    def edge_copy(d):
        slot = 1 - d
        return pltpu.make_async_remote_copy(
            src_ref=merged.at[1], dst_ref=merged.at[slot], send_sem=x3_send.at[slot],
            recv_sem=x3_recv.at[slot], device_id={"rows": r + d}, device_id_type=MESH,
        )

    for d in (1, -1):
        pl.when(there(d))(lambda d=d: edge_copy(d).start())

    if stages:
        hear(len(stages) - 1)

    def peak_copy(k):
        peer = lax.rem(me + k, n)
        return pltpu.make_async_remote_copy(
            src_ref=pk_send, dst_ref=pk_recv.at[k], send_sem=pk_ssem.at[k], recv_sem=pk_rsem.at[k],
            device_id={"rows": peer // T, "tm": lax.rem(peer, T)}, device_id_type=MESH,
        )

    def send_peak(k, carry):
        peak_copy(k).start()
        return carry

    lax.fori_loop(1, n, send_peak, 0, unroll=n <= 16)

    loads[3].wait()
    C2 = dec_ref.shape[2]
    width = frames * cols
    own = dot_nt(up[...], block).reshape(3, 3, C2, width)
    upper = own[1] + own[2]
    lower = own[0] + own[1]
    for d in (1, -1):
        pl.when(there(d))(lambda d=d: edge_copy(-d).wait_recv())
    upper = upper + dot_nt(up[0 : 3 * C2], merged[0].reshape(width, C)).reshape(3, C2, width)
    lower = lower + dot_nt(up[6 * C2 :], merged[2].reshape(width, C)).reshape(3, C2, width)
    lane = lax.rem(lax.broadcasted_iota(jnp.int32, (C2, width), 1), cols)

    def columns(sums):
        from_left = jnp.where(lane == 0, 0.0, pltpu.roll(sums[0], 1, 1))
        from_right = jnp.where(lane == cols - 1, 0.0, pltpu.roll(sums[2], width - 1, 1))
        even = from_left + sums[1] + sums[2]
        odd = sums[0] + sums[1] + from_right
        return jnp.concatenate([even, odd], axis=1).astype(BF16)

    narrow = jnp.concatenate([columns(upper), columns(lower)], axis=0)
    q = lax.broadcasted_iota(jnp.int32, (2 * width, 2 * width), 0)
    o = lax.broadcasted_iota(jnp.int32, (2 * width, 2 * width), 1)
    frame = lax.rem(lax.div(q, cols), frames)
    target = frame * (2 * cols) + 2 * lax.rem(q, cols) + lax.div(q, width)
    spread = jnp.where(o == target, 1.0, 0.0).astype(BF16)
    wide = dot(narrow, spread).astype(BF16)
    for f in range(frames):
        for j in range(2):
            dec_ref[f, j] = wide[j * C2 : (j + 1) * C2, f * 2 * cols : (f + 1) * 2 * cols]

    def take_peak(k, best):
        peak_copy(k).wait_recv()
        return jnp.maximum(best, pk_recv[k])

    best = lax.fori_loop(1, n, take_peak, pk_send[...], unroll=n <= 16)
    for i in range(3):
        peaks_ref[i : i + 1, 0:half] = best[2 * i : 2 * i + 1, :]
        peaks_ref[i : i + 1, half:C] = best[2 * i + 1 : 2 * i + 2, 0 : C - half]

    def end_peak(k, carry):
        peak_copy(k).wait_send()
        return carry

    lax.fori_loop(1, n, end_peak, 0, unroll=n <= 16)
    for d in offsets:
        pl.when(there(d))(lambda d=d: row_copy(d).wait_send())
    for d in (1, -1):
        pl.when(there(d))(lambda d=d: edge_copy(d).wait_send())

    @pl.when(gives)
    def _():
        for d in [0] + offsets:
            pl.when(there(d))(lambda d=d: relay(REACH + d).wait_send())
        hand_on().wait_send()


def per_device(latent, gain_first, conv_first, gain_second, conv_second, conv_up):
    frames, rows, cols, C = latent.shape
    R, T = lax.axis_size("rows"), lax.axis_size("tm")
    C2 = conv_up.shape[2]
    n = R * T
    if rows != 1 or frames != 2:
        raise ValueError("unsupported block")
    half = 128
    depth = -(-C // 256) * 256
    taps = 27
    vmem = pl.BlockSpec(memory_space=pltpu.VMEM)
    hbm = pl.BlockSpec(memory_space=pl.ANY)
    dma = pltpu.SemaphoreType.DMA
    return pl.pallas_call(
        functools.partial(kernel, R, T),
        out_shape=(
            jax.ShapeDtypeStruct((frames, 2 * rows, C2, 2 * cols), BF16),
            jax.ShapeDtypeStruct((3, C), F32),
        ),
        in_specs=[hbm, vmem, hbm, vmem, hbm, hbm],
        out_specs=(vmem, vmem),
        scratch_shapes=[
            pltpu.VMEM((2 * REACH + 1, frames, cols, C), BF16),
            pltpu.VMEM((2 * REACH + 1, frames, cols, C), BF16),
            pltpu.VMEM((2 * frames, (2 * REACH + 1) * cols, depth), BF16),
            pltpu.VMEM((2 * frames, 3 * cols, depth), BF16),
            pltpu.VMEM((taps, depth, C), BF16),
            pltpu.VMEM((taps, depth, C), BF16),
            pltpu.VMEM((9 * C2, C), BF16),
            pltpu.VMEM((3, frames, cols, C), BF16),
            pltpu.VMEM((8, half), F32),
            pltpu.VMEM((n, 8, half), F32),
            dma((4,)),
            dma((2 * REACH + 1,)),
            dma((2 * REACH + 1,)),
            dma((2 * REACH + 1,)),
            dma((2 * REACH + 1,)),
            dma,
            dma,
            dma((3,)),
            dma((3,)),
            dma((n,)),
            dma((n,)),
            pltpu.SemaphoreType.REGULAR((R.bit_length(), 2)),
        ],
        compiler_params=pltpu.CompilerParams(collective_id=0, has_side_effects=True),
    )(
        latent.reshape(frames, cols, C),
        gain_first,
        conv_first.reshape(taps, C, C),
        gain_second,
        conv_second.reshape(taps, C, C),
        conv_up.reshape(9 * C2, C),
    )


def solution(mesh):
    return jax.shard_map(
        per_device,
        mesh=mesh,
        in_specs=(P(("clip", "tm"), "rows", None, None), P(), P(), P(), P(), P()),
        out_specs=(P(("clip", "tm"), "rows", None, None), P("clip", None)),
        check_vma=False,
    )
```

```python
import functools

import jax
import jax.numpy as jnp
from jax import lax
from jax.experimental import pallas as pl
from jax.experimental.pallas import tpu as pltpu
from jax.sharding import PartitionSpec as P

MESH = pl.DeviceIdType.MESH
BF16 = jnp.bfloat16
F32 = jnp.float32
REACH = 2


def normed_silu(values, gain):
    scale = lax.rsqrt(jnp.mean(values * values, axis=-1, keepdims=True) + 1e-06)
    u = values * scale * gain
    return (u / (1.0 + jnp.exp(-u))).astype(BF16)


def peak_of(values):
    return jnp.max(jnp.abs(values.astype(F32)), axis=0, keepdims=True)


def dot(a, b):
    return jnp.dot(a, b, preferred_element_type=F32)


def dot_nt(a, b):
    return lax.dot_general(a, b, (((1,), (1,)), ((), ())), preferred_element_type=F32)


def taps_part(buf, weights, time_taps, frames, rows_out, cols):
    depth = buf.shape[-1]
    pixels = frames * rows_out * cols
    pairs = [(i, j) for i in time_taps for j in range(3)]
    lhs = jnp.concatenate(
        [
            buf[i : i + frames, j * cols : (j + rows_out) * cols, :].reshape(pixels, depth)
            for i, j in pairs
        ],
        axis=1,
    )
    return [
        dot(lhs, jnp.concatenate([weights[(i * 3 + j) * 3 + k] for i, j in pairs], axis=0))
        for k in range(3)
    ]


def shifted_sum(parts, more, cols):
    parts = [a + b for a, b in zip(parts, more)]
    pixels = parts[0].shape[0]
    col = lax.rem(lax.broadcasted_iota(jnp.int32, parts[0].shape, 0), cols)
    left = jnp.where(col == 0, 0.0, pltpu.roll(parts[0], 1, 0))
    right = jnp.where(col == cols - 1, 0.0, pltpu.roll(parts[2], pixels - 1, 0))
    return left + parts[1] + right


def finish(dec_in, peaks_in, dec_out, peaks_out, sem):
    copies = [
        pltpu.make_async_copy(dec_in, dec_out, sem.at[0]),
        pltpu.make_async_copy(peaks_in, peaks_out, sem.at[1]),
    ]
    for copy in copies:
        copy.start()
    for copy in copies:
        copy.wait()


def kernel(
    R, T, lat_hbm, g1_ref, w1_hbm, g2_ref, w2_hbm, up_hbm, dec_ref, peaks_ref,
    lat, prev, first, second, w1, w2, up, merged, pk_send, pk_recv,
    load_sem, x1_send, x1_recv, rl_send, rl_recv, s_send, s_recv, x3_send, x3_recv, pk_ssem, pk_rsem, known, spread,
):
    r = lax.axis_index("rows")
    t = lax.axis_index("tm")
    n = R * T
    me = r * T + t
    _, frames, cols, C = lat.shape
    half = pk_send.shape[-1]
    SPAN = 2 * REACH + 1

    loads = [
        pltpu.make_async_copy(lat_hbm, lat.at[REACH], load_sem.at[0]),
        pltpu.make_async_copy(w1_hbm, w1.at[:, 0:C, :], load_sem.at[1]),
        pltpu.make_async_copy(w2_hbm, w2.at[:, 0:C, :], load_sem.at[2]),
        pltpu.make_async_copy(up_hbm, up, load_sem.at[3]),
    ]
    for copy in loads:
        copy.start()

    barrier = pltpu.get_barrier_semaphore()

    def there(d):
        return jnp.logical_and(r + d >= 0, r + d < R)

    near = [(d, e) for d in range(-REACH, REACH + 1) for e in range(T) if (d, e) != (0, 0)]

    def greet(d, e):
        pl.semaphore_signal(
            barrier, inc=1, device_id={"rows": r + d, "tm": lax.rem(t + e, T)}, device_id_type=MESH
        )

    second[frames:, :, :] = jnp.zeros_like(second[frames:, :, :])

    @pl.when(t == 0)
    def _():
        second[0:frames, :, :] = jnp.zeros_like(second[0:frames, :, :])

    @pl.when(r == 0)
    def _():
        merged[0] = jnp.zeros_like(merged[0])

    @pl.when(r == R - 1)
    def _():
        merged[2] = jnp.zeros_like(merged[2])

    for d, e in near:
        pl.when(there(d))(functools.partial(greet, d, e))

    first[...] = jnp.zeros_like(first)
    pad = w1.shape[1] - C
    w1[:, C:, :] = jnp.zeros((w1.shape[0], pad, C), BF16)
    w2[:, C:, :] = jnp.zeros((w2.shape[0], pad, C), BF16)
    pk_send[...] = jnp.zeros_like(pk_send)

    width = frames * cols
    q = lax.broadcasted_iota(jnp.int32, (2 * width, 2 * width), 0)
    o = lax.broadcasted_iota(jnp.int32, (2 * width, 2 * width), 1)
    frame = lax.rem(lax.div(q, cols), frames)
    target = frame * (2 * cols) + 2 * lax.rem(q, cols) + lax.div(q, width)
    spread[...] = jnp.where(o == target, 1.0, 0.0).astype(BF16)

    loads[0].wait()
    rows_near = 1 + jnp.minimum(r, REACH) + jnp.minimum(R - 1 - r, REACH)
    pl.semaphore_wait(barrier, rows_near * T - 1)

    offsets = [1, -1, 2, -2]

    def row_copy(d):
        slot = REACH - d
        return pltpu.make_async_remote_copy(
            src_ref=lat.at[REACH], dst_ref=lat.at[slot], send_sem=x1_send.at[slot],
            recv_sem=x1_recv.at[slot], device_id={"rows": r + d}, device_id_type=MESH,
        )

    for d in offsets:
        pl.when(there(d))(lambda d=d: row_copy(d).start())

    stages = [REACH << i for i in range(R.bit_length()) if (REACH << i) < R - 1]

    def tell(i):
        for side, d in enumerate((stages[i], -stages[i])):
            pl.when(there(d))(
                lambda side=side, d=d: pl.semaphore_signal(
                    known.at[i, side], inc=1, device_id={"rows": r + d}, device_id_type=MESH
                )
            )

    def hear(i):
        for side, d in enumerate((stages[i], -stages[i])):
            pl.when(there(-d))(lambda side=side: pl.semaphore_wait(known.at[i, side], 1))

    if stages:
        tell(0)

    def relay(slot):
        return pltpu.make_async_remote_copy(
            src_ref=lat.at[slot], dst_ref=prev.at[slot], send_sem=rl_send.at[slot],
            recv_sem=rl_recv.at[slot], device_id={"tm": t + 1}, device_id_type=MESH,
        )

    gives = t < T - 1
    takes = t > 0
    pl.when(gives)(lambda: relay(REACH).start())

    gain1 = g1_ref[...].astype(F32).reshape(1, C)
    gain2 = g2_ref[...].astype(F32).reshape(1, C)

    def put_first(source, slot, at):
        rows = slice(slot * cols, (slot + 1) * cols)
        values = normed_silu(source[slot].astype(F32).reshape(frames * cols, C), gain1)
        first[at : at + frames, rows, 0:C] = values.reshape(frames, cols, C)
        return values

    def put_peak(i, row):
        pk_send[2 * i : 2 * i + 1, :] = row[:, 0:half]
        pk_send[2 * i + 1 : 2 * i + 2, 0 : C - half] = row[:, half:C]

    put_peak(0, peak_of(put_first(lat, REACH, frames)))

    for d in offsets:
        slot = REACH + d

        @pl.when(there(d))
        def _(d=d, slot=slot):
            row_copy(-d).wait_recv()
            pl.when(gives)(lambda: relay(slot).start())
            put_first(lat, slot, frames)

    for i in range(1, len(stages)):
        hear(i - 1)
        tell(i)

    loads[1].wait()
    parts = taps_part(first, w1, (2,), frames, 3, cols)

    @pl.when(takes)
    def _():
        for d in [0] + offsets:
            slot = REACH + d

            @pl.when(there(d))
            def _(slot=slot):
                relay(slot).wait_recv()
                put_first(prev, slot, 0)

    more = taps_part(first, w1, (0, 1), frames, 3, cols)
    hidden = shifted_sum(parts, more, cols).astype(BF16).astype(F32)
    activated = normed_silu(hidden, gain2).reshape(frames, 3, cols, C)
    zeros = jnp.zeros((frames, cols, C), BF16)
    for j in range(3):
        values = activated[:, j]
        if j != 1:
            values = jnp.where(there(j - 1), values, zeros)
        second[frames:, j * cols : (j + 1) * cols, 0:C] = values

    def hand_on():
        return pltpu.make_async_remote_copy(
            src_ref=second.at[pl.ds(frames, frames)], dst_ref=second.at[pl.ds(0, frames)],
            send_sem=s_send, recv_sem=s_recv, device_id={"tm": t + 1}, device_id_type=MESH,
        )

    pl.when(gives)(lambda: hand_on().start())
    put_peak(1, peak_of(activated[:, 1].reshape(frames * cols, C)))
    loads[2].wait()
    parts = taps_part(second, w2, (2,), frames, 1, cols)
    pl.when(takes)(lambda: hand_on().wait_recv())

    more = taps_part(second, w2, (0, 1), frames, 1, cols)
    block = lat[REACH].astype(F32).reshape(frames * cols, C) + shifted_sum(parts, more, cols)
    block = block.astype(BF16)
    merged[1] = block.reshape(frames, cols, C)
    put_peak(2, peak_of(block))

    def edge_copy(d):
        slot = 1 - d
        return pltpu.make_async_remote_copy(
            src_ref=merged.at[1], dst_ref=merged.at[slot], send_sem=x3_send.at[slot],
            recv_sem=x3_recv.at[slot], device_id={"rows": r + d}, device_id_type=MESH,
        )

    for d in (1, -1):
        pl.when(there(d))(lambda d=d: edge_copy(d).start())

    if stages:
        hear(len(stages) - 1)

    def peak_copy(k):
        peer = lax.rem(me + k, n)
        return pltpu.make_async_remote_copy(
            src_ref=pk_send, dst_ref=pk_recv.at[k], send_sem=pk_ssem.at[k], recv_sem=pk_rsem.at[k],
            device_id={"rows": peer // T, "tm": lax.rem(peer, T)}, device_id_type=MESH,
        )

    def send_peak(k, carry):
        peak_copy(k).start()
        return carry

    lax.fori_loop(1, n, send_peak, 0, unroll=n <= 16)

    loads[3].wait()
    C2 = dec_ref.shape[2]
    own = dot_nt(up[...], block).reshape(3, 3, C2, width)
    upper = own[1] + own[2]
    lower = own[0] + own[1]
    for d in (1, -1):
        pl.when(there(d))(lambda d=d: edge_copy(-d).wait_recv())
    upper = upper + dot_nt(up[0 : 3 * C2], merged[0].reshape(width, C)).reshape(3, C2, width)
    lower = lower + dot_nt(up[6 * C2 :], merged[2].reshape(width, C)).reshape(3, C2, width)
    lane = lax.rem(lax.broadcasted_iota(jnp.int32, (C2, width), 1), cols)

    def columns(sums):
        from_left = jnp.where(lane == 0, 0.0, pltpu.roll(sums[0], 1, 1))
        from_right = jnp.where(lane == cols - 1, 0.0, pltpu.roll(sums[2], width - 1, 1))
        even = from_left + sums[1] + sums[2]
        odd = sums[0] + sums[1] + from_right
        return jnp.concatenate([even, odd], axis=1).astype(BF16)

    narrow = jnp.concatenate([columns(upper), columns(lower)], axis=0)
    wide = dot(narrow, spread[...]).astype(BF16)
    for f in range(frames):
        for j in range(2):
            dec_ref[f, j] = wide[j * C2 : (j + 1) * C2, f * 2 * cols : (f + 1) * 2 * cols]

    def take_peak(k, best):
        peak_copy(k).wait_recv()
        return jnp.maximum(best, pk_recv[k])

    best = lax.fori_loop(1, n, take_peak, pk_send[...], unroll=n <= 16)
    for i in range(3):
        peaks_ref[i : i + 1, 0:half] = best[2 * i : 2 * i + 1, :]
        peaks_ref[i : i + 1, half:C] = best[2 * i + 1 : 2 * i + 2, 0 : C - half]

    def end_peak(k, carry):
        peak_copy(k).wait_send()
        return carry

    lax.fori_loop(1, n, end_peak, 0, unroll=n <= 16)
    for d in offsets:
        pl.when(there(d))(lambda d=d: row_copy(d).wait_send())
    for d in (1, -1):
        pl.when(there(d))(lambda d=d: edge_copy(d).wait_send())

    @pl.when(gives)
    def _():
        for d in [0] + offsets:
            pl.when(there(d))(lambda d=d: relay(REACH + d).wait_send())
        hand_on().wait_send()


def per_device(latent, gain_first, conv_first, gain_second, conv_second, conv_up):
    frames, rows, cols, C = latent.shape
    R, T = lax.axis_size("rows"), lax.axis_size("tm")
    C2 = conv_up.shape[2]
    n = R * T
    if rows != 1 or frames != 2:
        raise ValueError("unsupported block")
    half = 128
    depth = -(-C // 256) * 256
    taps = 27
    vmem = pl.BlockSpec(memory_space=pltpu.VMEM)
    hbm = pl.BlockSpec(memory_space=pl.ANY)
    dma = pltpu.SemaphoreType.DMA
    decoded, peaks = pl.pallas_call(
        functools.partial(kernel, R, T),
        out_shape=(
            jax.ShapeDtypeStruct((frames, 2 * rows, C2, 2 * cols), BF16),
            jax.ShapeDtypeStruct((3, C), F32),
        ),
        in_specs=[hbm, vmem, hbm, vmem, hbm, hbm],
        out_specs=(vmem, vmem),
        scratch_shapes=[
            pltpu.VMEM((2 * REACH + 1, frames, cols, C), BF16),
            pltpu.VMEM((2 * REACH + 1, frames, cols, C), BF16),
            pltpu.VMEM((2 * frames, (2 * REACH + 1) * cols, depth), BF16),
            pltpu.VMEM((2 * frames, 3 * cols, depth), BF16),
            pltpu.VMEM((taps, depth, C), BF16),
            pltpu.VMEM((taps, depth, C), BF16),
            pltpu.VMEM((9 * C2, C), BF16),
            pltpu.VMEM((3, frames, cols, C), BF16),
            pltpu.VMEM((8, half), F32),
            pltpu.VMEM((n, 8, half), F32),
            dma((4,)),
            dma((2 * REACH + 1,)),
            dma((2 * REACH + 1,)),
            dma((2 * REACH + 1,)),
            dma((2 * REACH + 1,)),
            dma,
            dma,
            dma((3,)),
            dma((3,)),
            dma((n,)),
            dma((n,)),
            pltpu.SemaphoreType.REGULAR((R.bit_length(), 2)),
            pltpu.VMEM((2 * frames * cols, 2 * frames * cols), BF16),
        ],
        compiler_params=pltpu.CompilerParams(collective_id=0, has_side_effects=True, vmem_limit_bytes=54 * 2**20),
    )(
        latent.reshape(frames, cols, C),
        gain_first,
        conv_first.reshape(taps, C, C),
        gain_second,
        conv_second.reshape(taps, C, C),
        conv_up.reshape(9 * C2, C),
    )
    return pl.pallas_call(
        finish,
        out_shape=(
            jax.ShapeDtypeStruct(decoded.shape, BF16),
            jax.ShapeDtypeStruct(peaks.shape, F32),
        ),
        in_specs=[vmem, vmem],
        out_specs=(hbm, hbm),
        scratch_shapes=[dma((2,))],
    )(decoded, peaks)


def solution(mesh):
    return jax.shard_map(
        per_device,
        mesh=mesh,
        in_specs=(P(("clip", "tm"), "rows", None, None), P(), P(), P(), P(), P()),
        out_specs=(P(("clip", "tm"), "rows", None, None), P("clip", None)),
        check_vma=False,
    )
```
